32 devices in a mesh: row: 8 (over z, x), col: 4 (over y, core).
Axes of the slice: x: 2, y: 2, z: 4, core: 2. Of those that a mesh axis runs over, the one named last changes fastest.
Arguments:
- positions: float32 [3, 24576], P(None, ('row', 'col')), may hold values from -0.5 to 209.5, as said below
- widths: float32 [24576], P(('row', 'col')), may hold values from 0.8 to 1.6
- hardness: float32 [24576], P(('row', 'col')), may hold values from 16 to 48
- right_sides: float32 [64, 24576], P(None, ('row', 'col')), may hold values from -700 to 700
Outputs:
- charges: float32 [64, 24576], P(None, ('row', 'col'))
- residual: float32 [64, 24576], P(None, ('row', 'col'))
The draws below stay inside these ranges and needn't reach their ends.
Inputs may be any that keep to these rules, and one draw needn't show every extreme that they name: `positions`: atoms sit near distinct sites of a lattice of spacing 2.2; any two atoms are 1.2 or more apart.
All inputs are finite; a program needn't handle non-finite values.
Results may differ from the reference program's by a relative error of at most 0.0003.
Values sent between devices are 32-bit elements; how exact they have to be, the bound alone decides.
No kernel may reach another device: no remote copies, remote signals or barrier semaphores. Data moves between devices by JAX's collectives and lax.ppermute only.
A program may use at most 128 MiB of HBM per device.

```python
import math
import jax
import jax.numpy as jnp
from jax import lax

ATOMS = 24576
RHS = 64
ITERS = 6


def draw_positions(key, part):
    lattice_site = jax.random.permutation(jax.random.fold_in(key, 11), ATOMS).astype(jnp.int32)
    grid_x = lattice_site % 16
    grid_y = lattice_site // 16 % 16
    grid_z = lattice_site // 256
    lattice = jnp.stack([grid_x, grid_y, grid_z]).astype(jnp.float32) * 2.2
    jitter = jax.random.uniform(jax.random.fold_in(key, 12), (3, ATOMS), jnp.float32, -0.4, 0.4)
    return lattice + jitter


def draw_right_sides(key, part):
    normal_part = jnp.clip(jax.random.normal(jax.random.fold_in(key, 21), (RHS, ATOMS), jnp.float32), -4.0, 4.0)
    rising = jnp.exp(jnp.log(3.0) * jnp.arange(ATOMS).astype(jnp.float32) / ATOMS)
    atom_scale = jnp.exp(jax.random.uniform(jax.random.fold_in(key, 23), (ATOMS,), jnp.float32, 0.0, jnp.log(10.0)))
    return 2.0 * normal_part * (atom_scale * rising)[None, :]


def shard_levels(rng, dims, pieces, low, high):
    gain, own = 1.0, jax.random.fold_in(rng, 6)
    for axis_at, blocks in pieces:
        steps = jnp.exp(jax.random.uniform(jax.random.fold_in(own, axis_at), (blocks,), jnp.float32, low / len(pieces), high / len(pieces)))
        gain = gain * jnp.repeat(steps, dims[axis_at] // blocks).reshape([-1 if axis == axis_at else 1 for axis in range(len(dims))])
    return gain


def setup_inputs(seed: int = 0) -> dict:
    key_of = jax.random.split(jax.random.key(seed), 5)
    positions = draw_positions(jax.random.fold_in(key_of[4], 71), 0)
    widths = jnp.clip(jnp.exp(math.log(1.6) - 0.6931472 * jax.random.uniform(key_of[1], (ATOMS,), jnp.float32) ** shard_levels(key_of[1], (ATOMS,), ((0, 32),), -0.2, 0.2)), 0.8, 1.6)
    hardness = jnp.clip(jnp.exp(math.log(48.0) - 1.0986123 * jax.random.uniform(key_of[2], (ATOMS,), jnp.float32) ** shard_levels(key_of[2], (ATOMS,), ((0, 32),), -0.2, 0.2)), 16.0, 48.0)
    right_sides = draw_right_sides(jax.random.fold_in(key_of[4], 71), 0)
    return {"positions": positions, "widths": widths, "hardness": hardness, "right_sides": right_sides}


root_two = 1.4142135623730951
sqrt_pi = 1.7724538509055159

def kernel_block(pos_a, wid_a, pos_b, wid_b):
    squared = jnp.zeros((pos_a.shape[1], pos_b.shape[1]), jnp.float32)
    for axis_id in range(3):
        delta = pos_a[axis_id][:, None] - pos_b[axis_id][None, :]
        squared = squared + delta * delta
    distinct = squared > 0.25
    distance = jnp.sqrt(jnp.maximum(squared, 0.25))
    width_pair = jnp.sqrt(wid_a[:, None] * wid_a[:, None] + wid_b[None, :] * wid_b[None, :])
    coulomb = lax.erf(distance / (root_two * width_pair)) / distance
    return jnp.where(distinct, coulomb, 0.0)

def apply_matrix(search, positions, widths, diagonal):
    block_count = ATOMS // 256
    pos_blocks = jnp.transpose(positions.reshape(3, block_count, 256), (1, 0, 2))
    wid_blocks = widths.reshape(block_count, 256)

    def column_block(pair):
        pos_block, wid_block = pair
        coupling = kernel_block(positions, widths, pos_block, wid_block)
        return jnp.dot(search, coupling, precision=lax.Precision.HIGHEST, preferred_element_type=jnp.float32)
    blocks_out = lax.map(column_block, (pos_blocks, wid_blocks))
    mapped = jnp.transpose(blocks_out, (1, 0, 2)).reshape(search.shape[0], ATOMS)
    return mapped + diagonal[None, :] * search

def reference(positions, widths, hardness, right_sides):
    diagonal = hardness + 1.0 / (widths * sqrt_pi)
    charges = jnp.zeros_like(right_sides)
    residual = right_sides
    search = right_sides
    norm_now = lax.optimization_barrier(jnp.sum(residual * residual, axis=1))
    for iteration in range(ITERS):
        mapped = apply_matrix(search, positions, widths, diagonal)
        step_len = norm_now / lax.optimization_barrier(jnp.sum(search * mapped, axis=1))
        charges = charges + step_len[:, None] * search
        residual = residual - step_len[:, None] * mapped
        norm_next = lax.optimization_barrier(jnp.sum(residual * residual, axis=1))
        search = residual + (norm_next / norm_now)[:, None] * search
        norm_now = norm_next
    return (charges, residual)
```

```python
import functools

import jax
import jax.numpy as jnp
from jax import lax
from jax.experimental import pallas as pl
from jax.experimental.pallas import tpu as pltpu
from jax.sharding import PartitionSpec as P

ITERS = 6
AXES = ("row", "col")
LOW_SCALE = 65536.0
LOW_TYPE = jnp.float8_e4m3fn
STRIP = 32
KERNEL_VMEM = 3 * 512 * 1024
SMALL_VMEM = 512 * 1024

root_half = 0.7071067811865476
sqrt_pi = 1.7724538509055159


def inner_factor(rows):
    best = 1
    for k in range(1, rows + 1):
        if rows % k == 0 and k * k <= rows:
            best = k
    return best


class Layout:
    def __init__(self, rows, cols):
        self.X = inner_factor(rows)
        self.Z = rows // self.X
        self.Y = cols // 2
        self.rows, self.cols = rows, cols

    def shift(self, array, dz=0, dx=0, dy=0, dc=0):
        pairs = []
        for r in range(self.rows):
            for c in range(self.cols):
                z, x, y, k = r // self.X, r % self.X, c // 2, c % 2
                to_row = (z ^ dz) * self.X + (x ^ dx)
                to_col = (y ^ dy) * 2 + (k ^ dc)
                pairs.append((r * self.cols + c, to_row * self.cols + to_col))
        return lax.ppermute(array, AXES, pairs)

    def planar(self):
        return [(dx, dy) for dx in range(self.X) for dy in range(self.Y)]

    def from_plane(self, array):
        return [array if d == (0, 0) else self.shift(array, dx=d[0], dy=d[1]) for d in self.planar()]

    def from_depth(self, array):
        return [array if k == 0 else self.shift(array, dz=k) for k in range(self.Z)]


def coulomb(xj, yj, zj, wj, xi, yi, zi, wi):
    dx, dy, dz = xj - xi, yj - yi, zj - zi
    squared = dx * dx + dy * dy + dz * dz
    inverse = lax.rsqrt(jnp.maximum(squared, 0.25))
    scale = lax.rsqrt(wj + wi)
    x = squared * inverse * scale
    t = 1.0 / (1.0 + 0.3275911 * x)
    poly = t * (0.254829592 + t * (-0.284496736 + t * (1.421413741 + t * (-1.453152027 + t * 1.061405429))))
    value = inverse - inverse * (poly * jnp.exp(-(x * x)))
    return jnp.where(squared > 0.25, value, 0.0)


def form_kernel(depth, pj_ref, pi_ref, *out_refs):
    cols, rows = out_refs[0].shape[1], pj_ref.shape[0]
    step = 256 if cols % 256 == 0 else cols
    base = pl.program_id(0) * rows

    def strip(s, carry):
        pj = pj_ref[pl.ds(pl.multiple_of(s * STRIP, STRIP), STRIP), :]
        at = pl.ds(pl.multiple_of(base + s * STRIP, STRIP), STRIP)
        for k in range(depth):
            for first in range(0, cols, step):
                lanes = slice(first, first + step)
                value = coulomb(
                    pj[:, 0:1], pj[:, 1:2], pj[:, 2:3], pj[:, 3:4],
                    pi_ref[k, 0:1, lanes], pi_ref[k, 1:2, lanes], pi_ref[k, 2:3, lanes], pi_ref[k, 3:4, lanes],
                )
                high = value.astype(jnp.bfloat16)
                low = (value - high.astype(jnp.float32)) * LOW_SCALE
                out_refs[k][at, lanes] = high
                out_refs[depth + k][at, lanes] = low.astype(LOW_TYPE)
        return carry

    lax.fori_loop(0, rows // STRIP, strip, 0)


def form(pj, pi):
    total, n, depth = pj.shape[0], pi.shape[2], pi.shape[0]
    out = pl.pallas_call(
        functools.partial(form_kernel, depth),
        grid=(total // n,),
        in_specs=[
            pl.BlockSpec((n, 8), lambda g: (g, 0)),
            pl.BlockSpec(pi.shape, lambda g: (0, 0, 0)),
        ],
        out_specs=[pl.BlockSpec(memory_space=pltpu.VMEM)] * (2 * depth),
        out_shape=[pltpu.VMEM((total, n), jnp.bfloat16)] * depth + [pltpu.VMEM((total, n), LOW_TYPE)] * depth,
        compiler_params=pltpu.CompilerParams(vmem_limit_bytes=KERNEL_VMEM),
        cost_estimate=pl.CostEstimate(flops=40 * depth * total * n, bytes_accessed=3 * depth * total * n, transcendentals=0),
        name="form_coupling",
    )(pj, pi)
    return out[:depth], out[depth:]


WHOLE = pl.BlockSpec(memory_space=pltpu.VMEM)


def resident(array):
    return pltpu.with_memory_space_constraint(array, pltpu.VMEM)


def small_call(kernel, out_shape, name, *operands, aliases=None):
    many = isinstance(out_shape, (list, tuple))
    size = sum(x.size * x.dtype.itemsize for x in operands)
    return pl.pallas_call(
        kernel,
        in_specs=[WHOLE] * len(operands),
        out_specs=[WHOLE] * len(out_shape) if many else WHOLE,
        out_shape=out_shape,
        input_output_aliases=aliases or {},
        compiler_params=pltpu.CompilerParams(vmem_limit_bytes=SMALL_VMEM),
        cost_estimate=pl.CostEstimate(flops=size, bytes_accessed=size, transcendentals=0),
        name=name,
    )(*operands)


def tree_sum(parts):
    while len(parts) > 1:
        parts = [parts[i] + parts[i + 1] for i in range(0, len(parts), 2)]
    return parts[0]


def stack_kernel(*refs):
    for i, ref in enumerate(refs[:-1]):
        refs[-1][i] = ref[...]


def stack(arrays):
    first = arrays[0]
    shape = jax.ShapeDtypeStruct((len(arrays), *first.shape), first.dtype)
    return small_call(stack_kernel, shape, "stack_plane", *arrays)


def add_kernel(*refs):
    refs[-1][...] = tree_sum([ref[...] for ref in refs[:-1]])


def add(arrays):
    return small_call(add_kernel, jax.ShapeDtypeStruct(arrays[0].shape, arrays[0].dtype), "add_sums", *arrays)


def write_pieces(pieces, first, value):
    rows, n = value.shape
    lanes = slice(first, first + n)
    high = value.astype(jnp.bfloat16)
    pieces[:rows, lanes] = high
    pieces[rows:, lanes] = (value - high.astype(jnp.float32)).astype(jnp.bfloat16)


def begin_kernel(a_ref, b_ref, residual, pieces):
    half, _, n = a_ref.shape
    for g in range(2 * half):
        value = a_ref[g] if g < half else b_ref[g - half]
        residual[g] = value
        write_pieces(pieces, g * n, value)


def begin(a, b):
    half, rows, n = a.shape
    shapes = [
        jax.ShapeDtypeStruct((2 * half, rows, n), jnp.float32),
        pltpu.VMEM((2 * rows, 2 * half * n), jnp.bfloat16),
    ]
    return small_call(begin_kernel, shapes, "begin_search", a, b)


def combine_kernel(depth, *refs):
    parts, (diag_ref, r_ref, s_ref, mapped_ref, sums_ref) = refs[:depth], refs[depth:]
    own_r, own_s = r_ref[0], s_ref[0]
    mapped = tree_sum([ref[...] for ref in parts]) + diag_ref[...] * own_s
    mapped_ref[...] = mapped
    rows = mapped.shape[0]
    lane = lax.broadcasted_iota(jnp.int32, (rows, 128), 1)
    table = jnp.zeros((rows, 128), jnp.float32)
    for i, value in enumerate((own_r * own_r, own_s * mapped, own_r * mapped, mapped * mapped)):
        table = jnp.where(lane == i, jnp.sum(value, axis=1, keepdims=True), table)
    table = jnp.concatenate([table, jnp.zeros((128 - rows, 128), jnp.float32)], axis=0)
    sums_ref[...] = table.T[:8]


def combine(parts, diagonal, residual, search):
    rows, n = parts[0].shape
    shapes = [jax.ShapeDtypeStruct((rows, n), jnp.float32), jax.ShapeDtypeStruct((8, 128), jnp.float32)]
    kernel = functools.partial(combine_kernel, len(parts))
    return small_call(kernel, shapes, "combine_parts", *parts, diagonal, residual, search)


def columns(sums, rows):
    table = jnp.concatenate([sums, jnp.zeros((120, 128), jnp.float32)], axis=0).T[:rows]
    return table[:, 0:1], table[:, 1:2], table[:, 2:3], table[:, 3:4]


def update_kernel(near_ref, far_ref, ma_ref, mb_ref, r_ref, s_ref, c_ref, r_out, s_out, c_out, pieces):
    half, rows, n = ma_ref.shape
    norm, bend, cross, square = columns(near_ref[...] + far_ref[...], rows)
    step = norm / bend
    norm_next = norm - 2.0 * step * cross + step * step * square
    turn = norm_next / norm
    for g in range(2 * half):
        search = s_ref[g]
        if g == 0:
            c_out[...] = c_ref[...] + step * search
        residual = r_ref[g] - step * (ma_ref[g] if g < half else mb_ref[g - half])
        search = residual + turn * search
        r_out[g] = residual
        s_out[g] = search
        write_pieces(pieces, g * n, search)


def update(near, far, ma, mb, residual, search, charges):
    half, rows, n = ma.shape
    shapes = [
        jax.ShapeDtypeStruct(residual.shape, jnp.float32),
        jax.ShapeDtypeStruct(search.shape, jnp.float32),
        jax.ShapeDtypeStruct(charges.shape, jnp.float32),
        pltpu.VMEM((2 * rows, 2 * half * n), jnp.bfloat16),
    ]
    return small_call(update_kernel, shapes, "update_search", near, far, ma, mb, residual, search, charges, aliases={4: 0, 5: 1, 6: 2})


def finish_kernel(near_ref, far_ref, m_ref, r_ref, s_ref, c_ref, c_out, r_out):
    norm, bend, _, _ = columns(near_ref[...] + far_ref[...], m_ref.shape[0])
    step = norm / bend
    c_out[...] = c_ref[...] + step * s_ref[0]
    r_out[...] = r_ref[0] - step * m_ref[...]


def finish(near, far, mapped, residual, search, charges):
    shapes = [jax.ShapeDtypeStruct(charges.shape, jnp.float32)] * 2
    return small_call(finish_kernel, shapes, "finish_charges", near, far, mapped, residual, search, charges)


def product_kernel(s_ref, hi_ref, lo_ref, out_ref):
    rows = out_ref.shape[0]
    dims = (((1,), (0,)), ((), ()))
    high = lax.dot_general(s_ref[...], hi_ref[...], dims, preferred_element_type=jnp.float32)
    low = lax.dot_general(s_ref[:rows], lo_ref[...], dims, preferred_element_type=jnp.float32)
    out_ref[...] = high[:rows] + high[rows:] + low * (1.0 / LOW_SCALE)


def product(pieces, hi, lo):
    rows2, total = pieces.shape
    rows, n = rows2 // 2, hi.shape[1]
    return pl.pallas_call(
        product_kernel,
        in_specs=[WHOLE] * 3,
        out_specs=WHOLE,
        out_shape=jax.ShapeDtypeStruct((rows, n), jnp.float32),
        compiler_params=pltpu.CompilerParams(vmem_limit_bytes=KERNEL_VMEM),
        cost_estimate=pl.CostEstimate(flops=6 * rows * total * n, bytes_accessed=3 * total * n, transcendentals=0),
        name="product",
    )(resident(pieces), resident(hi), resident(lo))


def local(shape, positions, widths, hardness, right_sides):
    lay = Layout(*shape)
    n = widths.shape[0]
    diagonal = (hardness + 1.0 / (widths * sqrt_pi))[None, :]
    packed = jnp.concatenate(
        [positions, (2.0 * widths * widths)[None, :], jnp.zeros((4, n), jnp.float32)], axis=0
    )
    own = jnp.stack(lay.from_plane(packed))
    pj = jnp.concatenate([own, lay.shift(own, dc=1)])
    pj = jnp.transpose(pj, (0, 2, 1)).reshape(-1, 8)
    pi = jnp.stack(lay.from_depth(packed))
    own = stack(lay.from_plane(right_sides))
    residual, pieces = begin(own, lay.shift(own, dc=1))
    search = residual
    charges = jnp.zeros_like(right_sides)

    hi, lo = form(pj, pi)
    for iteration in range(ITERS):
        parts = {}
        for k in reversed(range(lay.Z)):
            partial = product(pieces, hi[k], lo[k])
            parts[k] = partial if k == 0 else lay.shift(partial, dz=k)
        mapped, sums = combine([parts[k] for k in range(lay.Z)], diagonal, residual, search)
        last = iteration == ITERS - 1
        if not last:
            ma = stack(lay.from_plane(mapped))
            mb = lay.shift(ma, dc=1)
        near = add(lay.from_plane(add(lay.from_depth(sums))))
        far = lay.shift(near, dc=1)
        if last:
            return finish(near, far, mapped, residual, search, charges)
        residual, search, charges, pieces = update(near, far, ma, mb, residual, search, charges)


def solution(mesh):
    in_specs = (P(None, AXES), P(AXES), P(AXES), P(None, AXES))
    out_specs = (P(None, AXES), P(None, AXES))
    body = functools.partial(local, (mesh.shape["row"], mesh.shape["col"]))
    return jax.shard_map(body, mesh=mesh, in_specs=in_specs, out_specs=out_specs, check_vma=False)
```

```python
import functools

import jax
import jax.numpy as jnp
from jax import lax
from jax.experimental import pallas as pl
from jax.experimental.pallas import tpu as pltpu
from jax.sharding import PartitionSpec as P


ITERS = 6
AXES = ("row", "col")
LOW_SCALE = 65536.0
LOW_TYPE = jnp.float8_e4m3fn
STRIP = 32
UNROLL = 8
KERNEL_VMEM = 3 * 512 * 1024
SMALL_VMEM = 6 * 1024 * 1024
STREAM_VMEM = 10 * 1024 * 1024
FORM_VMEM = 5 * 1024 * 1024

sqrt_pi = 1.7724538509055159


def inner_factor(rows):
    best = 1
    for k in range(1, rows + 1):
        if rows % k == 0 and k * k <= rows:
            best = k
    return best


class Layout:
    def __init__(self, rows, cols):
        self.X = inner_factor(rows)
        self.Z = rows // self.X
        self.Y = cols // 2
        self.rows, self.cols = rows, cols

    def shift(self, array, dz=0, dx=0, dy=0, dc=0):
        pairs = []
        for r in range(self.rows):
            for c in range(self.cols):
                z, x, y, k = r // self.X, r % self.X, c // 2, c % 2
                to_row = (z ^ dz) * self.X + (x ^ dx)
                to_col = (y ^ dy) * 2 + (k ^ dc)
                pairs.append((r * self.cols + c, to_row * self.cols + to_col))
        return lax.ppermute(array, AXES, pairs)

    def planar(self):
        return [(dx, dy) for dx in range(self.X) for dy in range(self.Y)]

    def from_plane(self, array):
        return [array if d == (0, 0) else self.shift(array, dx=d[0], dy=d[1]) for d in self.planar()]

    def from_depth(self, array):
        return [array if k == 0 else self.shift(array, dz=k) for k in range(self.Z)]


WHOLE = pl.BlockSpec(memory_space=pltpu.VMEM)


ERFC_LOG2 = (-1.627831032, -0.9187606773, -0.1482958361, 0.02936798642, -0.002897739958)
STRETCH = (-ERFC_LOG2[4]) ** 0.2


def coulomb(pj, pi, masked):
    dx, dy, dz = pj[0] - pi[0], pj[1] - pi[1], pj[2] - pi[2]
    squared = dx * dx + dy * dy + dz * dz
    least = 0.25 / (LOW_SCALE * LOW_SCALE)
    inverse = lax.rsqrt(jnp.maximum(squared, least) if masked else squared)
    x = (squared * inverse) * lax.rsqrt(pj[3] + pi[3])
    power = ERFC_LOG2[3] / STRETCH ** 4 - x
    for k in (3, 2, 1):
        power = power * x + ERFC_LOG2[k - 1] / STRETCH ** k
    value = inverse - inverse * jnp.exp2(power * x)
    return jnp.where(squared > least, value, 0.0) if masked else value


def form_kernel(masked, pj_ref, pi_ref, hi_ref, lo_ref):
    cols, rows = hi_ref.shape[1], pj_ref.shape[0]
    step = tile_width(cols)
    windowed = hi_ref.shape[0] == rows
    base = 0 if windowed else pl.program_id(0) * rows

    strips = rows // STRIP
    together = UNROLL if strips % UNROLL == 0 else 1

    def strip(mask, s, carry):
        for u in range(together):
            first_row = (s * together + u) * STRIP
            pj = pj_ref[pl.ds(pl.multiple_of(first_row, STRIP), STRIP), :]
            at = pl.ds(pl.multiple_of(base + first_row, STRIP), STRIP)
            columns_j = [pj[:, c:c + 1] for c in range(4)]
            for first in range(0, cols, step):
                lanes = slice(first, first + step)
                value = coulomb(columns_j, [pi_ref[c:c + 1, lanes] for c in range(4)], mask)
                high = value.astype(jnp.bfloat16)
                hi_ref[at, lanes] = high
                lo_ref[at, lanes] = (value - high.astype(jnp.float32)).astype(LOW_TYPE)
        return carry

    def run(mask):
        lax.fori_loop(0, strips // together, functools.partial(strip, mask), 0)

    if not masked:
        run(False)
        return

    @pl.when(pl.program_id(0) == 0)
    def _():
        run(True)

    @pl.when(pl.program_id(0) > 0)
    def _():
        run(False)


def form(pj, pi, k):
    total, n = pj.shape[0], pi.shape[1]
    space, spec = (pltpu.VMEM, WHOLE) if k else (pltpu.HBM, pl.BlockSpec((n, n), lambda g: (g, 0)))
    return pl.pallas_call(
        functools.partial(form_kernel, k == 0),
        grid=(total // n,),
        in_specs=[pl.BlockSpec((n, 8), lambda g: (g, 0)), WHOLE],
        out_specs=[spec, spec],
        out_shape=[space((total, n), jnp.bfloat16), space((total, n), LOW_TYPE)],
        compiler_params=pltpu.CompilerParams(vmem_limit_bytes=FORM_VMEM),
        cost_estimate=pl.CostEstimate(flops=40 * total * n, bytes_accessed=3 * total * n, transcendentals=0),
        name="form_coupling",
    )(pj, pi)


def resident(array):
    return pltpu.with_memory_space_constraint(array, pltpu.VMEM)


def small_call(kernel, out_shape, *operands, aliases=None):
    many = isinstance(out_shape, (list, tuple))
    size = sum(x.size * x.dtype.itemsize for x in operands)
    return pl.pallas_call(
        kernel,
        in_specs=[WHOLE] * len(operands),
        out_specs=[WHOLE] * len(out_shape) if many else WHOLE,
        out_shape=out_shape,
        input_output_aliases=aliases or {},
        compiler_params=pltpu.CompilerParams(vmem_limit_bytes=SMALL_VMEM),
        cost_estimate=pl.CostEstimate(flops=size, bytes_accessed=size, transcendentals=0),
    )(*operands)


def tree_sum(parts):
    while len(parts) > 1:
        parts = [parts[i] + parts[i + 1] for i in range(0, len(parts), 2)]
    return parts[0]


def stack_kernel(*refs):
    for i, ref in enumerate(refs[:-1]):
        refs[-1][i] = ref[...]


def stack(arrays):
    first = arrays[0]
    shape = jax.ShapeDtypeStruct((len(arrays), *first.shape), first.dtype)
    return small_call(stack_kernel, shape, *arrays)


def add_kernel(*refs):
    refs[-1][...] = tree_sum([ref[...] for ref in refs[:-1]])


def add(arrays):
    return small_call(add_kernel, jax.ShapeDtypeStruct(arrays[0].shape, arrays[0].dtype), *arrays)


def write_pieces(pieces, first, value):
    rows, n = value.shape
    lanes = slice(first, first + n)
    high = value.astype(jnp.bfloat16)
    pieces[:rows, lanes] = high
    pieces[rows:, lanes] = (value - high.astype(jnp.float32)).astype(jnp.bfloat16)


def begin_kernel(a_ref, b_ref, residual, pieces):
    half, _, n = a_ref.shape
    for g in range(2 * half):
        value = a_ref[g] if g < half else b_ref[g - half]
        residual[g] = value
        write_pieces(pieces, g * n, value)


def begin(a, b):
    half, rows, n = a.shape
    shapes = [
        jax.ShapeDtypeStruct((2 * half, rows, n), jnp.float32),
        pltpu.VMEM((2 * rows, 2 * half * n), jnp.bfloat16),
    ]
    return small_call(begin_kernel, shapes, a, b)


def combine_kernel(depth, *refs):
    parts, (packed_ref, r_ref, s_ref, mapped_ref, sums_ref) = refs[:depth], refs[depth:]
    own_r, own_s = r_ref[0], s_ref[0]
    mapped = tree_sum([ref[...] for ref in parts]) + packed_ref[4:5, :] * own_s
    mapped_ref[...] = mapped
    rows = mapped.shape[0]
    lane = lax.broadcasted_iota(jnp.int32, (rows, 128), 1)
    table = jnp.zeros((rows, 128), jnp.float32)
    for i, value in enumerate((own_r * own_r, own_s * mapped, own_r * mapped, mapped * mapped)):
        table = jnp.where(lane == i, jnp.sum(value, axis=1, keepdims=True), table)
    table = jnp.concatenate([table, jnp.zeros((128 - rows, 128), jnp.float32)], axis=0)
    sums_ref[...] = table.T[:8]


def combine(parts, packed, residual, search):
    rows, n = parts[0].shape
    shapes = [jax.ShapeDtypeStruct((rows, n), jnp.float32), jax.ShapeDtypeStruct((8, 128), jnp.float32)]
    kernel = functools.partial(combine_kernel, len(parts))
    return small_call(kernel, shapes, *parts, packed, residual, search)


def columns(sums, rows):
    table = jnp.concatenate([sums, jnp.zeros((120, 128), jnp.float32)], axis=0).T[:rows]
    return table[:, 0:1], table[:, 1:2], table[:, 2:3], table[:, 3:4]


def update_kernel(first, near_ref, far_ref, ma_ref, mb_ref, r_ref, s_ref, *refs):
    c_ref, (r_out, s_out, c_out, pieces) = refs[0], refs[-4:]
    half, rows, n = ma_ref.shape
    norm, bend, cross, square = columns(near_ref[...] + far_ref[...], rows)
    step = norm / bend
    norm_next = norm - 2.0 * step * cross + step * step * square
    turn = norm_next / norm
    for g in range(2 * half):
        search = s_ref[g]
        if g == 0:
            c_out[...] = step * search if first else c_ref[...] + step * search
        residual = r_ref[g] - step * (ma_ref[g] if g < half else mb_ref[g - half])
        search = residual + turn * search
        r_out[g] = residual
        s_out[g] = search
        write_pieces(pieces, g * n, search)


def update(near, far, ma, mb, residual, search, charges):
    half, rows, n = ma.shape
    first = charges is None
    shapes = [
        jax.ShapeDtypeStruct(residual.shape, jnp.float32),
        jax.ShapeDtypeStruct(search.shape, jnp.float32),
        jax.ShapeDtypeStruct((rows, n), jnp.float32),
        pltpu.VMEM((2 * rows, 2 * half * n), jnp.bfloat16),
    ]
    operands = (near, far, ma, mb, residual, search) + (() if first else (charges,))
    aliases = {4: 0} if first else {4: 0, 5: 1, 6: 2}
    return small_call(functools.partial(update_kernel, first), shapes, *operands, aliases=aliases)


def finish_kernel(near_ref, far_ref, m_ref, r_ref, s_ref, c_ref, c_out, r_out):
    norm, bend, _, _ = columns(near_ref[...] + far_ref[...], m_ref.shape[0])
    step = norm / bend
    c_out[...] = c_ref[...] + step * s_ref[0]
    r_out[...] = r_ref[0] - step * m_ref[...]


def finish(near, far, mapped, residual, search, charges):
    shapes = [jax.ShapeDtypeStruct(charges.shape, jnp.float32)] * 2
    return small_call(finish_kernel, shapes, near, far, mapped, residual, search, charges)


def product_kernel(streamed, s_ref, hi_ref, lo_ref, out_ref):
    rows, n = out_ref.shape
    step = lo_ref.shape[1] if streamed else tile_width(n)
    dims = (((1,), (0,)), ((), ()))

    def tile(t, carry):
        lanes = pl.ds(pl.multiple_of(t * step, step), step) if step != n else slice(None)
        part = slice(None) if streamed else lanes
        high = lax.dot_general(s_ref[...], hi_ref[:, part], dims, preferred_element_type=jnp.float32)
        low = lax.dot_general(s_ref[:rows], lo_ref[:, part], dims, preferred_element_type=jnp.float32)
        out_ref[:, lanes] = (high[:rows] + high[rows:] + low) * (1.0 / LOW_SCALE)
        return carry

    if streamed:
        tile(pl.program_id(0), 0)
    else:
        lax.fori_loop(0, n // step, tile, 0)


def tile_width(n):
    return 256 if n % 256 == 0 else n


def product(pieces, hi, lo, streamed):
    rows2, total = pieces.shape
    rows, n = rows2 // 2, hi.shape[1]
    step = tile_width(n)
    spec = pl.BlockSpec((total, step), lambda t: (0, t)) if streamed else WHOLE
    place = functools.partial(pltpu.with_memory_space_constraint, memory_space=pltpu.HBM if streamed else pltpu.VMEM)
    return pl.pallas_call(
        functools.partial(product_kernel, streamed),
        grid=(n // step,) if streamed else (),
        in_specs=[WHOLE, spec, spec],
        out_specs=WHOLE,
        out_shape=jax.ShapeDtypeStruct((rows, n), jnp.float32),
        compiler_params=pltpu.CompilerParams(vmem_limit_bytes=STREAM_VMEM if streamed else KERNEL_VMEM),
        cost_estimate=pl.CostEstimate(flops=6 * rows * total * n, bytes_accessed=3 * total * n, transcendentals=0),
        name="product",
    )(resident(pieces), place(hi), place(lo))


def local(shape, positions, widths, hardness, right_sides):
    lay = Layout(*shape)
    n = widths.shape[0]
    packed = jnp.concatenate(
        [
            positions * (1.0 / LOW_SCALE),
            (2.0 / (LOW_SCALE * STRETCH) ** 2 * widths * widths)[None, :],
            (hardness + 1.0 / (widths * sqrt_pi))[None, :],
            jnp.zeros((3, n), jnp.float32),
        ],
        axis=0,
    )
    own = lay.from_plane(packed)
    own = jnp.stack(own)
    pj = jnp.concatenate([own, lay.shift(own, dc=1)])
    pi = lay.from_depth(packed)
    pj = jnp.transpose(pj, (0, 2, 1)).reshape(-1, 8)
    own = lay.from_plane(right_sides)
    own = stack(own)
    other = lay.shift(own, dc=1)
    residual, pieces = begin(own, other)
    search = residual
    charges = None
    coupling = {}

    for iteration in range(ITERS):
        last = iteration == ITERS - 1
        parts = {}
        for k in reversed(range(lay.Z)):
            if iteration == 0:
                coupling[k] = form(pj, pi[k], k)
            parts[k] = product(pieces, *coupling[k], k == 0)
            if k:
                parts[k] = lay.shift(parts[k], dz=k)
        mapped, sums = combine([parts[k] for k in range(lay.Z)], packed, residual, search)
        sums = lay.from_depth(sums)
        sums = add(sums)
        sums = lay.from_plane(sums)
        near = add(sums)
        far = lay.shift(near, dc=1)
        if last:
            return finish(near, far, mapped, residual, search, charges)
        gathered = lay.from_plane(mapped)
        ma = stack(gathered)
        mb = lay.shift(ma, dc=1)
        residual, search, charges, pieces = update(near, far, ma, mb, residual, search, charges)


def solution(mesh):
    in_specs = (P(None, AXES), P(AXES), P(AXES), P(None, AXES))
    out_specs = (P(None, AXES), P(None, AXES))
    shape = (mesh.shape["row"], mesh.shape["col"])
    body = functools.partial(local, shape)
    return jax.shard_map(body, mesh=mesh, in_specs=in_specs, out_specs=out_specs, check_vma=False)
```
